32 devices in a mesh: row: 8 (over z, core), col: 4 (over y, x).
Axes of the slice: x: 2, y: 2, z: 4, core: 2. Of those that a mesh axis runs over, the one named last changes fastest.
Arguments:
- vectors: bfloat16 [2, 4, 16384], P(None, 'col', 'row'), may hold values from -6 to 6
- lr_left: bfloat16 [8, 4, 32, 8, 2048], P('row', 'col'), may hold values from -0.75 to 0.75
- lr_right: bfloat16 [8, 4, 32, 8, 2048], P('row', 'col'), may hold values from -0.125 to 0.125
- tile_rank: int32 [8, 4, 32], P('row', 'col'), may hold values from 0 to 8, as said below
- leaf_values: bfloat16 [8, 4, 8, 512, 512], P('row', 'col'), may hold values from -0.25 to 0.25
- leaf_places: int32 [8, 4, 8, 2], P('row', 'col'), may hold values from 0 to 31, as said below
- cluster_perm: int32 [8, 8192], P('row'), may hold values from 0 to 65535, as said below
- kappa: float32 [32, 16, 128], P('row', 'col'), may hold values from 0.25 to 4
Outputs:
- prior_action: float32 [2, 32, 16, 128], P(None, 'row', 'col')
The draws below stay inside these ranges and needn't reach their ends.
Inputs may be any that keep to these rules, and one draw needn't show every extreme that they name: `tile_rank`: 0 exactly on the tiles that contain a leaf, 1 to 8 on the others. `leaf_places`: the 8 leaves of a block are distinct; entry 0 indexes rows and entry 1 column of the block in units of 512. `cluster_perm`: a permutation of all brick indices; within each aligned block of 2048 entries, every value of entry // 2048 occurs exactly 128 times or not at all.
All inputs are finite; a program needn't handle non-finite values.
Results may differ from the reference program's by a relative error of at most 0.0023.
Values may be sent and summed in bfloat16 or wider, within the bound.
A program may use at most 64 MiB of HBM per device.

```python
import math
import jax
import jax.numpy as jnp
from jax import lax

NVEC = 2
CX = 4
CY = 4
NZ = 128
TILE_ROWS = 4
TILE_COLS = 8
KMAX = 8
LEAF = 512
NLEAF = 8
PTS_DEV = 2048
BLOCK_ROWS = 8
BLOCK_COLS = 4
ROWS_CL = 8192
COLS_CL = 16384
TS = 2048
NX = 32
NY = 16
POINTS = 65536
CAP = 128
DEVICES = 32


def leaf_layout(key):
    base = jax.random.fold_in(key, 11)
    row_count = ROWS_CL // LEAF
    col_count = COLS_CL // LEAF
    every_key = jax.random.split(base, BLOCK_ROWS * BLOCK_COLS)

    def one_block(single):
        chosen = jax.random.permutation(single, row_count * col_count)[:NLEAF]
        return jnp.stack([chosen // col_count, chosen % col_count], axis=1)
    places = jax.vmap(one_block)(every_key)
    return places.reshape(BLOCK_ROWS, BLOCK_COLS, NLEAF, 2).astype(jnp.int32)


def draw_leaf_places(key, part):
    return leaf_layout(key)


def draw_tile_rank(key, part):
    places = leaf_layout(key)
    tile_ranks = jax.random.randint(jax.random.fold_in(key, 12), (BLOCK_ROWS, BLOCK_COLS, TILE_ROWS * TILE_COLS), 1, KMAX + 1)
    tile_of = places[..., 0] * LEAF // TS * TILE_COLS + places[..., 1] * LEAF // TS
    near_tile = jnp.any(tile_of[..., :, None] == jnp.arange(TILE_ROWS * TILE_COLS)[None, None, None, :], axis=2)
    return jnp.where(near_tile, 0, tile_ranks).astype(jnp.int32)


def draw_cluster_perm(key, part):
    base = jax.random.fold_in(key, 21)
    keys_a, keys_b, keys_c = jax.random.split(base, 3)
    group_total = PTS_DEV // CAP
    offsets = jax.random.permutation(keys_a, DEVICES)[:group_total]
    shuffle = jax.vmap(lambda single: jax.random.permutation(single, PTS_DEV))(jax.random.split(keys_b, DEVICES))
    landing = jax.vmap(lambda single: jax.random.permutation(single, PTS_DEV))(jax.random.split(keys_c, DEVICES))
    source = jnp.arange(DEVICES)[:, None]
    group_id = shuffle // CAP
    target = (source + offsets[group_id]) % DEVICES
    landing_spot = landing[target, shuffle]
    return (target * PTS_DEV + landing_spot).reshape(BLOCK_ROWS, ROWS_CL).astype(jnp.int32)


def levels(own_key, shape, shards, least, largest):
    gain, own = 1.0, jax.random.fold_in(own_key, 6)
    for axis_at, blocks in shards:
        heights = jnp.exp(jax.random.uniform(jax.random.fold_in(own, axis_at), (blocks,), jnp.float32, least / len(shards), largest / len(shards)))
        gain = gain * jnp.repeat(heights, shape[axis_at] // blocks).reshape([-1 if axis == axis_at else 1 for axis in range(len(shape))])
    return gain


def noise(rng, dims, scale, limit, shards=(), held_as=jnp.bfloat16):
    drawn = scale * jax.random.normal(rng, dims, jnp.float32)
    if shards:
        drawn = drawn * levels(rng, dims, shards, -0.22, 0.18)
    return jnp.clip(drawn, -limit, limit).astype(held_as)


def setup_inputs(seed: int = 0) -> dict:
    key_list = jax.random.split(jax.random.key(seed), 9)
    return {
        "vectors": noise(key_list[0], (NVEC, BLOCK_COLS, COLS_CL), 1.0, 6.0, ((1, 4), (2, 8))),
        "lr_left": noise(key_list[1], (BLOCK_ROWS, BLOCK_COLS, TILE_ROWS * TILE_COLS, KMAX, TS), (KMAX * TILE_COLS) ** -0.5, 0.75, ((0, 8), (1, 4))),
        "lr_right": noise(key_list[2], (BLOCK_ROWS, BLOCK_COLS, TILE_ROWS * TILE_COLS, KMAX, TS), TS ** -0.5, 0.125, ((0, 8), (1, 4))),
        "tile_rank": draw_tile_rank(jax.random.fold_in(key_list[8], 71), 0),
        "leaf_values": noise(key_list[4], (BLOCK_ROWS, BLOCK_COLS, NLEAF, LEAF, LEAF), LEAF ** -0.5, 0.25, ((0, 8), (1, 4))),
        "leaf_places": draw_leaf_places(jax.random.fold_in(key_list[8], 71), 0),
        "cluster_perm": draw_cluster_perm(jax.random.fold_in(key_list[8], 71), 0),
        "kappa": jnp.clip(jnp.exp(math.log(4.0) - 2.7725887 * jax.random.uniform(key_list[7], (NX, NY, NZ), jnp.float32) ** levels(key_list[7], (NX, NY, NZ), ((0, 8), (1, 4)), -0.2, 0.2)), 0.25, 4.0),
    }


def prior_step(padded, stiffness):
    center = padded[:, 1:-1, 1:-1, :]
    flat_pad = jnp.pad(center, ((0, 0), (0, 0), (0, 0), (1, 1)))
    beside = padded[:, 2:, 1:-1, :] + padded[:, :-2, 1:-1, :]
    beside = beside + padded[:, 1:-1, 2:, :] + padded[:, 1:-1, :-2, :]
    beside = beside + flat_pad[..., 2:] + flat_pad[..., :-2]
    return ((6.0 + stiffness) * center - beside) * 0.125


def block_product(far_left, far_right, tile_ranks, leaf_vals, leaf_pos, x_column):
    x_tiles = x_column.reshape(NVEC, TILE_COLS, TS).astype(jnp.float32)
    right_tiles = far_right.reshape(TILE_ROWS, TILE_COLS, KMAX, TS).astype(jnp.float32)
    projected = jnp.einsum('abkp,vbp->abvk', right_tiles, x_tiles)
    rank_mask = (jnp.arange(KMAX)[None, None, :] < tile_ranks.reshape(TILE_ROWS, TILE_COLS)[:, :, None]).astype(jnp.float32)
    projected = lax.optimization_barrier((projected * rank_mask[:, :, None, :]).astype(jnp.bfloat16)).astype(jnp.float32)
    left_tiles = far_left.reshape(TILE_ROWS, TILE_COLS, KMAX, TS).astype(jnp.float32)
    far_part = jnp.einsum('abkp,abvk->vap', left_tiles, projected).reshape(NVEC, ROWS_CL)
    x_sub = x_column.reshape(NVEC, COLS_CL // LEAF, LEAF).astype(jnp.float32)
    picked = x_sub[:, leaf_pos[:, 1], :]
    near_out = jnp.einsum('lqp,vlp->vlq', leaf_vals.astype(jnp.float32), picked)
    near_part = jnp.zeros((NVEC, ROWS_CL // LEAF, LEAF), jnp.float32).at[:, leaf_pos[:, 0], :].add(near_out)
    return far_part + near_part.reshape(NVEC, ROWS_CL)


def reference(vectors, lr_left, lr_right, tile_rank, leaf_values, leaf_places, cluster_perm, kappa):
    columns = jnp.transpose(vectors, (1, 0, 2))

    def one_row(inputs):
        left_row, right_row, rank_row, vals_row, pos_row = inputs

        def add_block(carry, column):
            left_one, right_one, rank_one, vals_one, pos_one, x_one = column
            return carry + block_product(left_one, right_one, rank_one, vals_one, pos_one, x_one), None

        summed, unused = lax.scan(add_block, jnp.zeros((NVEC, ROWS_CL), jnp.float32),
                                  (left_row, right_row, rank_row, vals_row, pos_row, columns))
        return summed

    sums = lax.map(one_row, (lr_left, lr_right, tile_rank, leaf_values, leaf_places))
    action = jnp.transpose(sums, (1, 0, 2)).reshape(NVEC, POINTS)
    bricks = jnp.zeros((NVEC, POINTS), jnp.float32).at[:, cluster_perm.reshape(-1)].set(action)
    field = bricks.reshape(NVEC, BLOCK_ROWS, BLOCK_COLS, CX, CY, NZ)
    field = jnp.transpose(field, (0, 1, 3, 2, 4, 5)).reshape(NVEC, NX, NY, NZ)
    for repeat in range(4):
        padded = jnp.pad(field, ((0, 0), (1, 1), (1, 1), (0, 0)))
        field = prior_step(padded, kappa)
    return field
```

```python
import functools

import jax
import jax.numpy as jnp
from jax import lax
from jax.experimental import pallas as pl
from jax.experimental.pallas import tpu as pltpu
from jax.sharding import PartitionSpec as P

CX = 4
CY = 4
TILE_ROWS = 4
TILE_COLS = 8
LANES = 128
MESH = pl.DeviceIdType.MESH
F32 = jnp.float32
BF16 = jnp.bfloat16
NT = (((1,), (1,)), ((), ()))
SIDES = [(a, b) for a in (-1, 0, 1) for b in (-1, 0, 1) if (a, b) != (0, 0)]


def dot_nt(a, b):
    return lax.dot_general(a, b, NT, preferred_element_type=F32)


def pieces(x):
    first = x.astype(BF16).astype(F32)
    rest = x - first
    second = rest.astype(BF16).astype(F32)
    return first, second, rest - second


def iota(shape, dim):
    return lax.broadcasted_iota(jnp.int32, shape, dim)


def kernel(
    rows, cols, kmax, leaf,
    x_ref, right_hbm, left_hbm, rank_ref, leaf_hbm, places_ref, perm_ref, kappa_ref,
    out_ref,
    right_ref, left_ref, leaf_ref, xg, x32, part, rs, slot_hot,
    msend, rm, vsend, rv, lane_hot, brick, hb, kb, ext, coef, scale,
    local_sem, ag_sem, m_sem, rs_sem, v_sem, k_send, k_recv, h_send, h_recv,
):
    nvec, points = x_ref.shape
    tile = right_ref.shape[1]
    taps = right_ref.shape[0]
    devices = rows * cols
    nleaf = leaf_ref.shape[0]
    cells = CX * CY
    blocks = points // LANES
    r = lax.axis_index("row")
    c = lax.axis_index("col")
    me = r * cols + c

    loads = [
        pltpu.make_async_copy(right_hbm, right_ref, local_sem.at[0]),
        pltpu.make_async_copy(left_hbm, left_ref, local_sem.at[1]),
        pltpu.make_async_copy(leaf_hbm, leaf_ref, local_sem.at[2]),
    ]
    for load in loads:
        load.start()

    def at(flat):
        return {"row": flat // cols, "col": flat % cols}

    barrier = pltpu.get_barrier_semaphore()

    def greet(k, carry):
        pl.semaphore_signal(
            barrier, inc=1, device_id=at(lax.rem(me + k, devices)), device_id_type=MESH
        )
        return carry

    lax.fori_loop(1, devices, greet, 0)

    targets = perm_ref[pl.ds(pl.multiple_of(c * blocks, 8), blocks), :]
    dev_of = targets // points
    place = targets % points
    place_hi = (place // LANES).astype(F32)
    place_lo = (place % LANES).astype(F32)
    dev_ids = iota((devices, LANES), 0)
    hots = [(dev_of[b : b + 1, :] == dev_ids).astype(F32) for b in range(blocks)]
    before = (iota((LANES, LANES), 0) < iota((LANES, LANES), 1)).astype(BF16)
    all_hot = jnp.concatenate(hots, axis=0).astype(BF16)
    inside = jnp.dot(all_hot, before, preferred_element_type=F32)
    totals = jnp.dot(all_hot, jnp.ones((LANES, LANES), BF16), preferred_element_type=F32)
    offset = jnp.zeros((devices, LANES), F32)
    lane_rows = iota((LANES, LANES), 0).astype(F32)
    for b in range(blocks):
        span = slice(b * devices, (b + 1) * devices)
        rank = jnp.sum(hots[b] * (inside[span] + offset), axis=0, keepdims=True)
        offset = offset + totals[span]
        slot_hot[:, b * LANES : (b + 1) * LANES] = (rank == lane_rows).astype(BF16)
    meta = jnp.concatenate(
        [
            jnp.concatenate(
                [hots[b] * place_hi[b : b + 1, :], hots[b] * place_lo[b : b + 1, :]], axis=0
            ).astype(BF16)
            for b in range(blocks)
        ],
        axis=1,
    )
    meta = dot_nt(meta, slot_hot[...])
    for h in range(2):
        msend[:, h, :] = meta[h * devices : (h + 1) * devices]

    xg[r] = x_ref[...]
    ext[...] = jnp.zeros_like(ext)
    coef[...] = jnp.zeros_like(coef)
    scale[...] = jnp.zeros_like(scale)
    pl.semaphore_wait(barrier, devices - 1)

    def spread(k, carry):
        pltpu.make_async_remote_copy(
            src_ref=x_ref, dst_ref=xg.at[r], send_sem=ag_sem.at[0], recv_sem=ag_sem.at[1],
            device_id={"row": lax.rem(r + k, rows), "col": c}, device_id_type=MESH,
        ).start()
        return carry

    lax.fori_loop(1, rows, spread, 0)

    def exchange(src, dst, sem):
        def send(k, carry):
            to = lax.rem(me + k, devices)
            pltpu.make_async_remote_copy(
                src_ref=src.at[to], dst_ref=dst.at[k - 1], send_sem=sem.at[0],
                recv_sem=sem.at[1], device_id=at(to), device_id_type=MESH,
            ).start()
            return carry

        lax.fori_loop(1, devices, send, 0)
        dst[devices - 1] = src[me]

    def settle(ref, count, sem):
        done = ref.at[pl.ds(0, count)]
        copy = pltpu.make_async_remote_copy(
            src_ref=done, dst_ref=done, send_sem=sem.at[0], recv_sem=sem.at[1],
            device_id=at(lax.rem(me + 1, devices)), device_id_type=MESH,
        )
        return copy

    def side(n):
        dr, dc = SIDES[n]
        rr, cc = r + dr, c + dc
        ok = (rr >= 0) & (rr < rows) & (cc >= 0) & (cc < cols)
        return ok, {"row": jnp.clip(rr, 0, rows - 1), "col": jnp.clip(cc, 0, cols - 1)}

    def side_copy(src, dst, send, recv, n, incoming):
        slot = n if incoming else len(SIDES) - 1 - n
        return pltpu.make_async_remote_copy(
            src_ref=src, dst_ref=dst.at[slot], send_sem=send.at[n], recv_sem=recv.at[slot],
            device_id=side(n)[1], device_id_type=MESH,
        )

    def sides_start(src, dst, send, recv):
        for n in range(len(SIDES)):
            @pl.when(side(n)[0])
            def _():
                side_copy(src, dst, send, recv, n, False).start()

    def sides_wait(src, dst, send, recv):
        for n in range(len(SIDES)):
            @pl.when(side(n)[0])
            def _():
                side_copy(src, dst, send, recv, n, True).wait_recv()
                side_copy(src, dst, send, recv, n, False).wait_send()

    exchange(msend, rm, m_sem)
    sides_start(kappa_ref, kb, k_send, k_recv)

    gathered = settle(xg, rows - 1, ag_sem)
    gathered.wait_recv()
    per = tile // points
    for s in range(rows):
        b, j = s // per, s % per
        x32[nvec * b : nvec * (b + 1), j * points : (j + 1) * points] = xg[s].astype(F32)
    loads[0].wait()
    wide = TILE_COLS * nvec
    projected = dot_nt(x32[...].astype(BF16), right_ref[...])
    lane = iota((1, taps), 1)
    lane_tile, lane_k = lane // kmax, lane % kmax
    ranks = jnp.zeros((1, taps), jnp.int32)
    for t in range(TILE_ROWS * TILE_COLS):
        ranks = jnp.where(lane_tile == t, rank_ref[t], ranks)
    keep = (lane_tile % TILE_COLS == iota((wide, taps), 0) // nvec) & (lane_k < ranks)
    projected = jnp.where(keep, projected, 0.0).astype(BF16)
    tall = TILE_ROWS * nvec
    fold = (iota((tall, wide), 0) % nvec == iota((tall, wide), 1) % nvec).astype(BF16)
    spread_out = jnp.dot(fold, projected, preferred_element_type=F32)
    own_row = lane_tile // TILE_COLS == iota((tall, taps), 0) // nvec
    spread_out = jnp.where(own_row, spread_out, 0.0).astype(BF16)
    loads[1].wait()
    far = jnp.dot(spread_out, left_ref[...], preferred_element_type=F32)
    loads[2].wait()
    subs = points // leaf
    near = []
    for l in range(nleaf):
        column = places_ref[2 * l + 1]
        held = xg[column // subs].astype(F32)
        sub = column % subs
        pick = jnp.zeros((nvec, leaf), F32)
        for q in range(subs):
            pick += jnp.where(sub == q, 1.0, 0.0) * held[:, q * leaf : (q + 1) * leaf]
        near.append(dot_nt(pick.astype(BF16), leaf_ref[l]))
    for d in range(cols):
        a, start = d * points // tile, d * points % tile
        for q in range(subs):
            total = far[nvec * a : nvec * (a + 1), start + q * leaf : start + (q + 1) * leaf]
            for l in range(nleaf):
                total += jnp.where(places_ref[2 * l] == d * subs + q, 1.0, 0.0) * near[l]
            part[d, :, q * leaf : (q + 1) * leaf] = total

    def share(k, carry):
        to = lax.rem(c + k, cols)
        pltpu.make_async_remote_copy(
            src_ref=part.at[to], dst_ref=rs.at[k - 1], send_sem=rs_sem.at[0],
            recv_sem=rs_sem.at[1], device_id={"row": r, "col": to}, device_id_type=MESH,
        ).start()
        return carry

    lax.fori_loop(1, cols, share, 0)

    sides_wait(kappa_ref, kb, k_send, k_recv)
    strip = 4 * CY

    def laid(ref, get, every):
        for n, (dr, dc) in enumerate(every):
            value = get(dr, dc)
            for x in range(CX):
                at_row = ((dr + 1) * CX + x) * strip + (dc + 1) * CY
                ref[at_row : at_row + CY, :] = value[x * CY : (x + 1) * CY, :]

    every = SIDES + [(0, 0)]

    def valid(dr, dc):
        return (r + dr >= 0) & (r + dr < rows) & (c + dc >= 0) & (c + dc < cols)

    def stiffness(dr, dc):
        if (dr, dc) == (0, 0):
            return (6.0 + kappa_ref[...]) * 0.125
        return jnp.where(valid(dr, dc), (6.0 + kb[SIDES.index((dr, dc))]) * 0.125, 0.0)

    laid(coef, stiffness, every)
    laid(
        scale,
        lambda dr, dc: jnp.full((cells, LANES), jnp.where(valid(dr, dc), 0.125, 0.0), F32),
        every,
    )
    metas = settle(rm, devices - 1, m_sem)
    metas.wait_recv()
    for s in range(devices):
        lane_hot[:, s * LANES : (s + 1) * LANES] = (rm[s, 1:2, :] == lane_rows).astype(BF16)

    shares = settle(rs, cols - 1, rs_sem)
    shares.wait_recv()
    action = part[c]
    for k in range(cols - 1):
        action += rs[k]

    terms = pieces(action)
    left_side = jnp.concatenate(
        [
            jnp.concatenate(
                [
                    jnp.where(
                        dev_of[b : b + 1, :] == dev_ids,
                        term[v : v + 1, b * LANES : (b + 1) * LANES],
                        0.0,
                    )
                    for term in terms
                    for v in range(nvec)
                ],
                axis=0,
            ).astype(BF16)
            for b in range(blocks)
        ],
        axis=1,
    )
    packed = dot_nt(left_side, slot_hot[...])
    size = nvec * devices
    packed = packed[:size] + packed[size : 2 * size] + packed[2 * size :]
    for v in range(nvec):
        vsend[:, v, :] = packed[v * devices : (v + 1) * devices]
    exchange(vsend, rv, v_sem)
    values = settle(rv, devices - 1, v_sem)
    values.wait_recv()

    cell_rows = iota((cells, LANES), 0).astype(F32)
    placed = []
    for s in range(devices):
        hit = rm[s, 0:1, :] == cell_rows
        bits = pieces(rv[s])
        placed.append(
            jnp.concatenate(
                [jnp.where(hit, bit[v : v + 1, :], 0.0) for bit in bits for v in range(nvec)],
                axis=0,
            ).astype(BF16)
        )
    field = dot_nt(jnp.concatenate(placed, axis=1), lane_hot[...])
    size = nvec * cells
    field = field[:size] + field[size : 2 * size] + field[2 * size :]
    for v in range(nvec):
        brick[v] = field[v * cells : (v + 1) * cells]
    sides_start(brick, hb, h_send, h_recv)
    gathered.wait_send()
    metas.wait_send()
    shares.wait_send()
    values.wait_send()
    sides_wait(brick, hb, h_send, h_recv)

    def bricks(v, dr, dc):
        if (dr, dc) == (0, 0):
            return brick[v]
        return jnp.where(valid(dr, dc), hb[SIDES.index((dr, dc)), v], 0.0)

    for v in range(nvec):
        laid(ext.at[v], functools.partial(bricks, v), every)
        cur = ext[v]
        for step in range(4):
            mid = cur[strip:-strip]
            z = iota(mid.shape, 1)
            beside = cur[2 * strip :] + cur[: -2 * strip]
            beside += pltpu.roll(mid, 1, 0) + pltpu.roll(mid, mid.shape[0] - 1, 0)
            beside += jnp.where(z > 0, pltpu.roll(mid, 1, 1), 0.0)
            beside += jnp.where(z < LANES - 1, pltpu.roll(mid, LANES - 1, 1), 0.0)
            low = (step + 1) * strip
            span = slice(low, ext.shape[1] - low)
            cur = coef[span, :] * mid - scale[span, :] * beside
        for x in range(CX):
            out_ref[v, x * CY : (x + 1) * CY, :] = cur[x * strip + CY : x * strip + 2 * CY]


def per_device(
    vectors, lr_left, lr_right, tile_rank, leaf_values, leaf_places, cluster_perm, kappa
):
    rows, cols = lax.axis_size("row"), lax.axis_size("col")
    devices = rows * cols
    nvec, _, points = vectors.shape
    tiles, kmax, tile = lr_left.shape[2:]
    nleaf, leaf = leaf_values.shape[2:4]
    cells, lanes = CX * CY, kappa.shape[2]
    taps = tiles * kmax
    strip, deep = 4 * CY, 3 * CX * 4 * CY
    vmem = pl.BlockSpec(memory_space=pltpu.VMEM)
    smem = pl.BlockSpec(memory_space=pltpu.SMEM)
    hbm = pl.BlockSpec(memory_space=pl.ANY)
    dma = pltpu.SemaphoreType.DMA
    out = pl.pallas_call(
        functools.partial(kernel, rows, cols, kmax, leaf),
        out_shape=jax.ShapeDtypeStruct((nvec, cells, lanes), F32),
        in_specs=[vmem, hbm, hbm, smem, hbm, smem, vmem, vmem],
        out_specs=vmem,
        scratch_shapes=[
            pltpu.VMEM((taps, tile), BF16),
            pltpu.VMEM((taps, tile), BF16),
            pltpu.VMEM((nleaf, leaf, leaf), BF16),
            pltpu.VMEM((rows, nvec, points), BF16),
            pltpu.VMEM((TILE_COLS * nvec, tile), F32),
            pltpu.VMEM((cols, nvec, points), F32),
            pltpu.VMEM((cols - 1, nvec, points), F32),
            pltpu.VMEM((LANES, points), BF16),
            pltpu.VMEM((devices, 2, LANES), F32),
            pltpu.VMEM((devices, 2, LANES), F32),
            pltpu.VMEM((devices, nvec, LANES), F32),
            pltpu.VMEM((devices, nvec, LANES), F32),
            pltpu.VMEM((LANES, devices * LANES), BF16),
            pltpu.VMEM((nvec, cells, lanes), F32),
            pltpu.VMEM((len(SIDES), nvec, cells, lanes), F32),
            pltpu.VMEM((len(SIDES), cells, lanes), F32),
            pltpu.VMEM((nvec, deep, lanes), F32),
            pltpu.VMEM((deep, lanes), F32),
            pltpu.VMEM((deep, lanes), F32),
            dma((3,)), dma((2,)), dma((2,)), dma((2,)), dma((2,)),
            dma((len(SIDES),)), dma((len(SIDES),)), dma((len(SIDES),)), dma((len(SIDES),)),
        ],
        compiler_params=pltpu.CompilerParams(collective_id=0, has_side_effects=True),
    )(
        vectors.reshape(nvec, points),
        lr_right.reshape(taps, tile),
        lr_left.reshape(taps, tile),
        tile_rank.reshape(tiles),
        leaf_values.reshape(nleaf, leaf, leaf),
        leaf_places.reshape(2 * nleaf),
        cluster_perm.reshape(-1, LANES),
        kappa.reshape(cells, lanes),
    )
    return out.reshape(nvec, CX, CY, lanes)


def solution(mesh):
    in_specs = (
        P(None, "col", "row"),
        P("row", "col", None, None, None),
        P("row", "col", None, None, None),
        P("row", "col", None),
        P("row", "col", None, None, None),
        P("row", "col", None, None),
        P("row", None),
        P("row", "col", None),
    )
    out_specs = P(None, "row", "col", None)
    return jax.shard_map(
        per_device, mesh=mesh, in_specs=in_specs, out_specs=out_specs, check_vma=False
    )
```

```python
import functools

import jax
import jax.numpy as jnp
from jax import lax
from jax.experimental import pallas as pl
from jax.experimental.pallas import tpu as pltpu
from jax.sharding import PartitionSpec as P

CX = 4
CY = 4
TILE_ROWS = 4
TILE_COLS = 8
LANES = 128
MESH = pl.DeviceIdType.MESH
F32 = jnp.float32
BF16 = jnp.bfloat16
NT = (((1,), (1,)), ((), ()))
SIDES = [(a, b) for a in (-1, 0, 1) for b in (-1, 0, 1) if (a, b) != (0, 0)]


def dot_nt(a, b):
    return lax.dot_general(a, b, NT, preferred_element_type=F32)


def pieces(x):
    first = x.astype(BF16).astype(F32)
    rest = x - first
    second = rest.astype(BF16).astype(F32)
    return first, second, rest - second


def iota(shape, dim):
    return lax.broadcasted_iota(jnp.int32, shape, dim)


def kernel(
    rows, cols, kmax, leaf,
    x_hbm, right_hbm, left_hbm, rank_ref, leaf_hbm, places_ref, perm_hbm, kappa_hbm,
    out_ref,
    perm_ref, kappa_ref, right_ref, left_ref, leaf_ref, xg, x32, part, rs, slot_hot,
    msend, rm, vsend, rv, lane_hot, brick, hb, kb, ext, coef, scale,
    local_sem, ag_sem, m_sem, rs_sem, v_sem, k_send, k_recv, h_send, h_recv,
):
    nvec, points = x_hbm.shape
    tile = right_ref.shape[1]
    taps = right_ref.shape[0]
    devices = rows * cols
    nleaf = leaf_ref.shape[0]
    cells = CX * CY
    blocks = points // LANES
    r = lax.axis_index("row")
    c = lax.axis_index("col")
    me = r * cols + c

    own_x = pltpu.make_async_copy(x_hbm, xg.at[r], local_sem.at[3])
    own_perm = pltpu.make_async_copy(
        perm_hbm.at[pl.ds(pl.multiple_of(c * blocks, 8), blocks)], perm_ref, local_sem.at[4]
    )
    own_kappa = pltpu.make_async_copy(kappa_hbm, kappa_ref, local_sem.at[5])
    loads = [
        pltpu.make_async_copy(right_hbm, right_ref, local_sem.at[0]),
        pltpu.make_async_copy(left_hbm, left_ref, local_sem.at[1]),
        pltpu.make_async_copy(leaf_hbm, leaf_ref, local_sem.at[2]),
    ]

    def turned(place, by, count):
        moved = place + by
        return moved - jnp.where(moved >= count, count, 0)

    barrier = pltpu.get_barrier_semaphore()
    for k in range(1, rows):
        pl.semaphore_signal(
            barrier, inc=1, device_id={"row": turned(r, k, rows), "col": c}, device_id_type=MESH
        )
    for k in range(1, cols):
        pl.semaphore_signal(
            barrier, inc=1, device_id={"row": r, "col": turned(c, k, cols)}, device_id_type=MESH
        )
    for load in [own_x, own_perm, own_kappa] + loads:
        load.start()
    own_x.wait()
    pl.semaphore_wait(barrier, rows + cols - 2)
    for k in range(1, rows):
        pltpu.make_async_remote_copy(
            src_ref=xg.at[r], dst_ref=xg.at[r], send_sem=ag_sem.at[0], recv_sem=ag_sem.at[1],
            device_id={"row": turned(r, k, rows), "col": c}, device_id_type=MESH,
        ).start()

    own_perm.wait()
    targets = perm_ref[...]
    dev_of = targets // points
    place = targets % points
    place_hi = (place // LANES).astype(F32)
    place_lo = (place % LANES).astype(F32)
    dev_ids = iota((devices, LANES), 0)
    hots = [(dev_of[b : b + 1, :] == dev_ids).astype(F32) for b in range(blocks)]
    before = (iota((LANES, LANES), 0) < iota((LANES, LANES), 1)).astype(BF16)
    all_hot = jnp.concatenate(hots, axis=0).astype(BF16)
    inside = jnp.dot(all_hot, before, preferred_element_type=F32)
    totals = jnp.dot(all_hot, jnp.ones((LANES, LANES), BF16), preferred_element_type=F32)
    offset = jnp.zeros((devices, LANES), F32)
    lane_rows = iota((LANES, LANES), 0).astype(F32)
    for b in range(blocks):
        span = slice(b * devices, (b + 1) * devices)
        rank = jnp.sum(hots[b] * (inside[span] + offset), axis=0, keepdims=True)
        offset = offset + totals[span]
        slot_hot[:, b * LANES : (b + 1) * LANES] = (rank == lane_rows).astype(BF16)
    meta = jnp.concatenate(
        [
            jnp.concatenate(
                [hots[b] * place_hi[b : b + 1, :], hots[b] * place_lo[b : b + 1, :]], axis=0
            ).astype(BF16)
            for b in range(blocks)
        ],
        axis=1,
    )
    meta = dot_nt(meta, slot_hot[...])
    for h in range(2):
        msend[:, h, :] = meta[h * devices : (h + 1) * devices]

    ext[...] = jnp.zeros_like(ext)
    coef[...] = jnp.zeros_like(coef)
    scale[...] = jnp.zeros_like(scale)

    def exchange(src, dst, sem):
        for dr in range(rows):
            for dc in range(cols):
                if dr + dc:
                    rr, cc = turned(r, dr, rows), turned(c, dc, cols)
                    pltpu.make_async_remote_copy(
                        src_ref=src.at[rr * cols + cc], dst_ref=dst.at[dr * cols + dc - 1],
                        send_sem=sem.at[0], recv_sem=sem.at[1],
                        device_id={"row": rr, "col": cc}, device_id_type=MESH,
                    ).start()
        dst[devices - 1] = src[me]

    def settle(ref, count, sem):
        done = ref.at[pl.ds(0, count)]
        copy = pltpu.make_async_remote_copy(
            src_ref=done, dst_ref=done, send_sem=sem.at[0], recv_sem=sem.at[1],
            device_id={"row": turned(r, 1, rows), "col": c}, device_id_type=MESH,
        )
        return copy

    def side(n):
        dr, dc = SIDES[n]
        rr, cc = r + dr, c + dc
        ok = (rr >= 0) & (rr < rows) & (cc >= 0) & (cc < cols)
        return ok, {"row": jnp.clip(rr, 0, rows - 1), "col": jnp.clip(cc, 0, cols - 1)}

    def side_copy(src, dst, send, recv, n, incoming):
        slot = n if incoming else len(SIDES) - 1 - n
        return pltpu.make_async_remote_copy(
            src_ref=src, dst_ref=dst.at[slot], send_sem=send.at[n], recv_sem=recv.at[slot],
            device_id=side(n)[1], device_id_type=MESH,
        )

    def sides_start(src, dst, send, recv):
        for n in range(len(SIDES)):
            @pl.when(side(n)[0])
            def _():
                side_copy(src, dst, send, recv, n, False).start()

    def sides_wait(src, dst, send, recv):
        for n in range(len(SIDES)):
            @pl.when(side(n)[0])
            def _():
                side_copy(src, dst, send, recv, n, True).wait_recv()
                side_copy(src, dst, send, recv, n, False).wait_send()

    gathered = settle(xg, rows - 1, ag_sem)
    gathered.wait_recv()
    per = tile // points
    for s in range(rows):
        b, j = s // per, s % per
        x32[nvec * b : nvec * (b + 1), j * points : (j + 1) * points] = xg[s].astype(F32)
    loads[0].wait()
    wide = TILE_COLS * nvec
    projected = dot_nt(x32[...].astype(BF16), right_ref[...])
    lane = iota((1, taps), 1)
    lane_tile, lane_k = lane // kmax, lane % kmax
    ranks = jnp.zeros((1, taps), jnp.int32)
    for t in range(TILE_ROWS * TILE_COLS):
        ranks = jnp.where(lane_tile == t, rank_ref[t], ranks)
    keep = (lane_tile % TILE_COLS == iota((wide, taps), 0) // nvec) & (lane_k < ranks)
    projected = jnp.where(keep, projected, 0.0).astype(BF16)
    tall = TILE_ROWS * nvec
    fold = (iota((tall, wide), 0) % nvec == iota((tall, wide), 1) % nvec).astype(BF16)
    spread_out = jnp.dot(fold, projected, preferred_element_type=F32)
    own_row = lane_tile // TILE_COLS == iota((tall, taps), 0) // nvec
    spread_out = jnp.where(own_row, spread_out, 0.0).astype(BF16)
    loads[1].wait()
    far = jnp.dot(spread_out, left_ref[...], preferred_element_type=F32)
    loads[2].wait()
    subs = points // leaf
    near = []
    for l in range(nleaf):
        column = places_ref[1, l]
        held = xg[column // subs].astype(F32)
        sub = column % subs
        pick = jnp.zeros((nvec, leaf), F32)
        for q in range(subs):
            pick += jnp.where(sub == q, 1.0, 0.0) * held[:, q * leaf : (q + 1) * leaf]
        near.append(dot_nt(pick.astype(BF16), leaf_ref[l]))
    for d in range(cols):
        a, start = d * points // tile, d * points % tile
        for q in range(subs):
            total = far[nvec * a : nvec * (a + 1), start + q * leaf : start + (q + 1) * leaf]
            for l in range(nleaf):
                total += jnp.where(places_ref[0, l] == d * subs + q, 1.0, 0.0) * near[l]
            part[d, :, q * leaf : (q + 1) * leaf] = total

    for k in range(1, cols):
        to = turned(c, k, cols)
        pltpu.make_async_remote_copy(
            src_ref=part.at[to], dst_ref=rs.at[k - 1], send_sem=rs_sem.at[0],
            recv_sem=rs_sem.at[1], device_id={"row": r, "col": to}, device_id_type=MESH,
        ).start()
    exchange(msend, rm, m_sem)
    own_kappa.wait()
    sides_start(kappa_ref, kb, k_send, k_recv)

    shares = settle(rs, cols - 1, rs_sem)
    shares.wait_recv()
    action = part[c]
    for k in range(cols - 1):
        action += rs[k]

    terms = pieces(action)
    left_side = jnp.concatenate(
        [
            jnp.concatenate(
                [
                    jnp.where(
                        dev_of[b : b + 1, :] == dev_ids,
                        term[v : v + 1, b * LANES : (b + 1) * LANES],
                        0.0,
                    )
                    for term in terms
                    for v in range(nvec)
                ],
                axis=0,
            ).astype(BF16)
            for b in range(blocks)
        ],
        axis=1,
    )
    packed = dot_nt(left_side, slot_hot[...])
    size = nvec * devices
    packed = packed[:size] + packed[size : 2 * size] + packed[2 * size :]
    for v in range(nvec):
        vsend[:, v, :] = packed[v * devices : (v + 1) * devices]
    exchange(vsend, rv, v_sem)
    sides_wait(kappa_ref, kb, k_send, k_recv)
    strip = 4 * CY

    def laid(ref, get, every):
        for n, (dr, dc) in enumerate(every):
            value = get(dr, dc)
            for x in range(CX):
                at_row = ((dr + 1) * CX + x) * strip + (dc + 1) * CY
                ref[at_row : at_row + CY, :] = value[x * CY : (x + 1) * CY, :]

    every = SIDES + [(0, 0)]

    def valid(dr, dc):
        return (r + dr >= 0) & (r + dr < rows) & (c + dc >= 0) & (c + dc < cols)

    def stiffness(dr, dc):
        if (dr, dc) == (0, 0):
            return (6.0 + kappa_ref[...]) * 0.125
        return jnp.where(valid(dr, dc), (6.0 + kb[SIDES.index((dr, dc))]) * 0.125, 0.0)

    laid(coef, stiffness, every)
    laid(
        scale,
        lambda dr, dc: jnp.full((cells, LANES), jnp.where(valid(dr, dc), 0.125, 0.0), F32),
        every,
    )
    metas = settle(rm, devices - 1, m_sem)
    metas.wait_recv()
    for s in range(devices):
        lane_hot[:, s * LANES : (s + 1) * LANES] = (rm[s, 1:2, :] == lane_rows).astype(BF16)

    values = settle(rv, devices - 1, v_sem)
    values.wait_recv()

    cell_rows = iota((cells, LANES), 0).astype(F32)
    placed = []
    for s in range(devices):
        hit = rm[s, 0:1, :] == cell_rows
        bits = pieces(rv[s])
        placed.append(
            jnp.concatenate(
                [jnp.where(hit, bit[v : v + 1, :], 0.0) for bit in bits for v in range(nvec)],
                axis=0,
            ).astype(BF16)
        )
    field = dot_nt(jnp.concatenate(placed, axis=1), lane_hot[...])
    size = nvec * cells
    field = field[:size] + field[size : 2 * size] + field[2 * size :]
    for v in range(nvec):
        brick[v] = field[v * cells : (v + 1) * cells]
    sides_start(brick, hb, h_send, h_recv)
    gathered.wait_send()
    metas.wait_send()
    shares.wait_send()
    values.wait_send()
    sides_wait(brick, hb, h_send, h_recv)

    def bricks(v, dr, dc):
        if (dr, dc) == (0, 0):
            return brick[v]
        return jnp.where(valid(dr, dc), hb[SIDES.index((dr, dc)), v], 0.0)

    for v in range(nvec):
        laid(ext.at[v], functools.partial(bricks, v), every)
        cur = ext[v]
        for step in range(4):
            mid = cur[strip:-strip]
            z = iota(mid.shape, 1)
            beside = cur[2 * strip :] + cur[: -2 * strip]
            beside += pltpu.roll(mid, 1, 0) + pltpu.roll(mid, mid.shape[0] - 1, 0)
            beside += jnp.where(z > 0, pltpu.roll(mid, 1, 1), 0.0)
            beside += jnp.where(z < LANES - 1, pltpu.roll(mid, LANES - 1, 1), 0.0)
            low = (step + 1) * strip
            span = slice(low, ext.shape[1] - low)
            cur = coef[span, :] * mid - scale[span, :] * beside
        out_ref[v] = cur.reshape(CX, strip, LANES)


def per_device(
    vectors, lr_left, lr_right, tile_rank, leaf_values, leaf_places, cluster_perm, kappa
):
    rows, cols = lax.axis_size("row"), lax.axis_size("col")
    devices = rows * cols
    nvec, _, points = vectors.shape
    tiles, kmax, tile = lr_left.shape[2:]
    nleaf, leaf = leaf_values.shape[2:4]
    cells, lanes = CX * CY, kappa.shape[2]
    taps = tiles * kmax
    strip, deep = 4 * CY, 3 * CX * 4 * CY
    vmem = pl.BlockSpec(memory_space=pltpu.VMEM)
    smem = pl.BlockSpec(memory_space=pltpu.SMEM)
    hbm = pl.BlockSpec(memory_space=pl.ANY)
    dma = pltpu.SemaphoreType.DMA
    out = pl.pallas_call(
        functools.partial(kernel, rows, cols, kmax, leaf),
        out_shape=jax.ShapeDtypeStruct((nvec, CX, strip, lanes), F32),
        in_specs=[hbm, hbm, hbm, smem, hbm, smem, hbm, hbm],
        out_specs=vmem,
        scratch_shapes=[
            pltpu.VMEM((points // LANES, LANES), jnp.int32),
            pltpu.VMEM((cells, lanes), F32),
            pltpu.VMEM((taps, tile), BF16),
            pltpu.VMEM((taps, tile), BF16),
            pltpu.VMEM((nleaf, leaf, leaf), BF16),
            pltpu.VMEM((rows, nvec, points), BF16),
            pltpu.VMEM((TILE_COLS * nvec, tile), F32),
            pltpu.VMEM((cols, nvec, points), F32),
            pltpu.VMEM((cols - 1, nvec, points), F32),
            pltpu.VMEM((LANES, points), BF16),
            pltpu.VMEM((devices, 2, LANES), F32),
            pltpu.VMEM((devices, 2, LANES), F32),
            pltpu.VMEM((devices, nvec, LANES), F32),
            pltpu.VMEM((devices, nvec, LANES), F32),
            pltpu.VMEM((LANES, devices * LANES), BF16),
            pltpu.VMEM((nvec, cells, lanes), F32),
            pltpu.VMEM((len(SIDES), nvec, cells, lanes), F32),
            pltpu.VMEM((len(SIDES), cells, lanes), F32),
            pltpu.VMEM((nvec, deep, lanes), F32),
            pltpu.VMEM((deep, lanes), F32),
            pltpu.VMEM((deep, lanes), F32),
            dma((6,)), dma((2,)), dma((2,)), dma((2,)), dma((2,)),
            dma((len(SIDES),)), dma((len(SIDES),)), dma((len(SIDES),)), dma((len(SIDES),)),
        ],
        compiler_params=pltpu.CompilerParams(collective_id=0, has_side_effects=True),
    )(
        vectors.reshape(nvec, points),
        lr_right.reshape(taps, tile),
        lr_left.reshape(taps, tile),
        tile_rank.reshape(tiles),
        leaf_values.reshape(nleaf, leaf, leaf),
        leaf_places.reshape(nleaf, 2).T,
        cluster_perm.reshape(-1, LANES),
        kappa.reshape(cells, lanes),
    )
    return out[:, :, CY : 2 * CY, :]


def solution(mesh):
    in_specs = (
        P(None, "col", "row"),
        P("row", "col", None, None, None),
        P("row", "col", None, None, None),
        P("row", "col", None),
        P("row", "col", None, None, None),
        P("row", "col", None, None),
        P("row", None),
        P("row", "col", None),
    )
    out_specs = P(None, "row", "col", None)
    return jax.shard_map(
        per_device, mesh=mesh, in_specs=in_specs, out_specs=out_specs, check_vma=False
    )
```

```python
import functools

import jax
import jax.numpy as jnp
from jax import lax
from jax.experimental import pallas as pl
from jax.experimental.pallas import tpu as pltpu
from jax.sharding import PartitionSpec as P

CX = 4
CY = 4
TILE_ROWS = 4
TILE_COLS = 8
LANES = 128
MESH = pl.DeviceIdType.MESH
F32 = jnp.float32
BF16 = jnp.bfloat16
NT = (((1,), (1,)), ((), ()))
SIDES = [(a, b) for a in (-1, 0, 1) for b in (-1, 0, 1) if (a, b) != (0, 0)]


def dot_nt(a, b):
    return lax.dot_general(a, b, NT, preferred_element_type=F32)


def pieces(x):
    first = x.astype(BF16).astype(F32)
    rest = x - first
    second = rest.astype(BF16).astype(F32)
    return first, second, rest - second


def iota(shape, dim):
    return lax.broadcasted_iota(jnp.int32, shape, dim)


def kernel(
    rows, cols, kmax, leaf,
    x_hbm, right_hbm, left_hbm, rank_hbm, leaf_hbm, places_hbm, perm_hbm, kappa_hbm,
    out_ref,
    rank_ref, places_ref, near_ref, corner, hc, perm_ref, kappa_ref, right_ref, left_ref, leaf_ref, xg, x32, part, rs, slot_hot,
    msend, rm, vsend, rv, lane_hot, brick, hb, kb, ext, coef, scale,
    local_sem, ag_sem, m_sem, rs_sem, v_sem, k_send, k_recv, h_send, h_recv,
):
    nvec, points = x_hbm.shape
    tile = right_ref.shape[1]
    taps = right_ref.shape[0]
    devices = rows * cols
    nleaf = leaf_ref.shape[0]
    cells = CX * CY
    blocks = points // LANES
    r = lax.axis_index("row")
    c = lax.axis_index("col")
    me = r * cols + c

    own_x = pltpu.make_async_copy(x_hbm, xg.at[r], local_sem.at[3])
    own_perm = pltpu.make_async_copy(
        perm_hbm.at[pl.ds(pl.multiple_of(c * blocks, 8), blocks)], perm_ref, local_sem.at[4]
    )
    own_kappa = pltpu.make_async_copy(kappa_hbm, kappa_ref, local_sem.at[5])
    small = [
        pltpu.make_async_copy(rank_hbm, rank_ref, local_sem.at[6]),
        pltpu.make_async_copy(places_hbm, places_ref, local_sem.at[7]),
    ]
    loads = [
        pltpu.make_async_copy(right_hbm, right_ref, local_sem.at[0]),
        pltpu.make_async_copy(left_hbm, left_ref, local_sem.at[1]),
        pltpu.make_async_copy(leaf_hbm, leaf_ref, local_sem.at[2]),
    ]

    def turned(place, by, count):
        moved = place + by
        return moved - jnp.where(moved >= count, count, 0)

    barrier = pltpu.get_barrier_semaphore()
    for k in range(1, rows):
        pl.semaphore_signal(
            barrier, inc=1, device_id={"row": turned(r, k, rows), "col": c}, device_id_type=MESH
        )
    for k in range(1, cols):
        pl.semaphore_signal(
            barrier, inc=1, device_id={"row": r, "col": turned(c, k, cols)}, device_id_type=MESH
        )
    for load in [own_x, own_perm] + small + [own_kappa] + loads:
        load.start()
    own_x.wait()
    pl.semaphore_wait(barrier, rows + cols - 2)
    for k in range(1, rows):
        pltpu.make_async_remote_copy(
            src_ref=xg.at[r], dst_ref=xg.at[r], send_sem=ag_sem.at[0], recv_sem=ag_sem.at[1],
            device_id={"row": turned(r, k, rows), "col": c}, device_id_type=MESH,
        ).start()

    own_perm.wait()
    targets = perm_ref[...]
    dev_of = targets // points
    place = targets % points
    place_hi = (place // LANES).astype(F32)
    place_lo = (place % LANES).astype(F32)
    dev_ids = iota((devices, LANES), 0)
    hots = [(dev_of[b : b + 1, :] == dev_ids).astype(F32) for b in range(blocks)]
    before = (iota((LANES, LANES), 0) < iota((LANES, LANES), 1)).astype(BF16)
    all_hot = jnp.concatenate(hots, axis=0).astype(BF16)
    inside = jnp.dot(all_hot, before, preferred_element_type=F32)
    totals = jnp.dot(all_hot, jnp.ones((LANES, LANES), BF16), preferred_element_type=F32)
    offset = jnp.zeros((devices, LANES), F32)
    lane_rows = iota((LANES, LANES), 0).astype(F32)
    for b in range(blocks):
        span = slice(b * devices, (b + 1) * devices)
        rank = jnp.sum(hots[b] * (inside[span] + offset), axis=0, keepdims=True)
        offset = offset + totals[span]
        slot_hot[:, b * LANES : (b + 1) * LANES] = (rank == lane_rows).astype(BF16)
    meta = jnp.concatenate(
        [
            jnp.concatenate(
                [hots[b] * place_hi[b : b + 1, :], hots[b] * place_lo[b : b + 1, :]], axis=0
            ).astype(BF16)
            for b in range(blocks)
        ],
        axis=1,
    )
    meta = dot_nt(meta, slot_hot[...])
    for h in range(2):
        msend[:, h, :] = meta[h * devices : (h + 1) * devices]

    for load in small:
        load.wait()
    wide = TILE_COLS * nvec
    lane = iota((1, taps), 1)
    lane_tile, lane_k = lane // kmax, lane % kmax
    ranks = jnp.zeros((1, taps), jnp.int32)
    for t in range(TILE_ROWS * TILE_COLS):
        ranks = jnp.where(lane_tile == t, rank_ref[t], ranks)
    keep = (lane_tile % TILE_COLS == iota((wide, taps), 0) // nvec) & (lane_k < ranks)
    tall = TILE_ROWS * nvec
    fold = (iota((tall, wide), 0) % nvec == iota((tall, wide), 1) % nvec).astype(BF16)
    own_row = lane_tile // TILE_COLS == iota((tall, taps), 0) // nvec
    picks = nleaf * nvec
    row_leaves = cols * points // leaf
    order = iota((1, 3 * picks), 1) % picks
    row_of = jnp.zeros((1, 3 * picks), jnp.int32)
    for l in range(nleaf):
        row_of = jnp.where(order // nvec == l, places_ref[0, l], row_of)
    chosen = iota((row_leaves * nvec, 3 * picks), 0)
    selector = ((chosen // nvec == row_of) & (chosen % nvec == order % nvec)).astype(BF16)

    ext[...] = jnp.zeros_like(ext)
    coef[...] = jnp.zeros_like(coef)
    scale[...] = jnp.zeros_like(scale)

    def exchange(src, dst, sem):
        for dr in range(rows):
            for dc in range(cols):
                if dr + dc:
                    rr, cc = turned(r, dr, rows), turned(c, dc, cols)
                    pltpu.make_async_remote_copy(
                        src_ref=src.at[rr * cols + cc], dst_ref=dst.at[dr * cols + dc - 1],
                        send_sem=sem.at[0], recv_sem=sem.at[1],
                        device_id={"row": rr, "col": cc}, device_id_type=MESH,
                    ).start()
        dst[devices - 1] = src[me]

    def settle(ref, count, sem):
        done = ref.at[pl.ds(0, count)]
        copy = pltpu.make_async_remote_copy(
            src_ref=done, dst_ref=done, send_sem=sem.at[0], recv_sem=sem.at[1],
            device_id={"row": turned(r, 1, rows), "col": c}, device_id_type=MESH,
        )
        return copy

    def side(n):
        dr, dc = SIDES[n]
        rr, cc = r + dr, c + dc
        ok = (rr >= 0) & (rr < rows) & (cc >= 0) & (cc < cols)
        return ok, {"row": jnp.clip(rr, 0, rows - 1), "col": jnp.clip(cc, 0, cols - 1)}

    def side_copy(pick, send, recv, n, incoming):
        slot = n if incoming else len(SIDES) - 1 - n
        src, dst = pick(n, slot)
        return pltpu.make_async_remote_copy(
            src_ref=src, dst_ref=dst, send_sem=send.at[n], recv_sem=recv.at[slot],
            device_id=side(n)[1], device_id_type=MESH,
        )

    def sides_start(pick, send, recv):
        for n in range(len(SIDES)):
            @pl.when(side(n)[0])
            def _():
                side_copy(pick, send, recv, n, False).start()

    def sides_wait(pick, send, recv):
        for n in range(len(SIDES)):
            @pl.when(side(n)[0])
            def _():
                side_copy(pick, send, recv, n, True).wait_recv()
                side_copy(pick, send, recv, n, False).wait_send()

    def kappa_sides(n, slot):
        return kappa_ref, kb.at[slot]

    def field_sides(n, slot):
        if 0 in SIDES[n]:
            return brick, hb.at[slot]
        return corner.at[n], hc.at[slot]

    def corner_cells(dr, dc):
        far_x = [CX - x if dr > 0 else x + 1 for x in range(CX)]
        far_y = [CY - y if dc > 0 else y + 1 for y in range(CY)]
        return [(x, y) for x in range(CX) for y in range(CY) if far_x[x] + far_y[y] <= 4]

    gathered = settle(xg, rows - 1, ag_sem)
    gathered.wait_recv()
    own_kappa.wait()
    sides_start(kappa_sides, k_send, k_recv)
    per = tile // points
    for s in range(rows):
        b, j = s // per, s % per
        x32[nvec * b : nvec * (b + 1), j * points : (j + 1) * points] = xg[s].astype(F32)
    loads[0].wait()
    projected = dot_nt(x32[...].astype(BF16), right_ref[...])
    projected = jnp.where(keep, projected, 0.0).astype(BF16)
    spread_out = jnp.dot(fold, projected, preferred_element_type=F32)
    spread_out = jnp.where(own_row, spread_out, 0.0).astype(BF16)
    loads[1].wait()
    far = jnp.dot(spread_out, left_ref[...], preferred_element_type=F32)
    loads[2].wait()
    subs = points // leaf
    for l in range(nleaf):
        column = places_ref[1, l]
        held = xg[column // subs].astype(F32)
        sub = column % subs
        pick = jnp.zeros((nvec, leaf), F32)
        for q in range(subs):
            pick += jnp.where(sub == q, 1.0, 0.0) * held[:, q * leaf : (q + 1) * leaf]
        near_ref[nvec * l : nvec * (l + 1), :] = dot_nt(pick.astype(BF16), leaf_ref[l])
    near = jnp.concatenate(pieces(near_ref[...]), axis=0).astype(BF16)
    near = jnp.dot(selector, near, preferred_element_type=F32)
    for d in range(cols):
        a, start = d * points // tile, d * points % tile
        for q in range(subs):
            at_row = nvec * (d * subs + q)
            part[d, :, q * leaf : (q + 1) * leaf] = (
                far[nvec * a : nvec * (a + 1), start + q * leaf : start + (q + 1) * leaf]
                + near[at_row : at_row + nvec]
            )
    for k in range(1, cols):
        to = turned(c, k, cols)
        pltpu.make_async_remote_copy(
            src_ref=part.at[to], dst_ref=rs.at[k - 1], send_sem=rs_sem.at[0],
            recv_sem=rs_sem.at[1], device_id={"row": r, "col": to}, device_id_type=MESH,
        ).start()
    exchange(msend, rm, m_sem)

    shares = settle(rs, cols - 1, rs_sem)
    shares.wait_recv()
    action = part[c]
    for k in range(cols - 1):
        action += rs[k]

    terms = pieces(action)
    left_side = jnp.concatenate(
        [
            jnp.concatenate(
                [
                    jnp.where(
                        dev_of[b : b + 1, :] == dev_ids,
                        term[v : v + 1, b * LANES : (b + 1) * LANES],
                        0.0,
                    )
                    for term in terms
                    for v in range(nvec)
                ],
                axis=0,
            ).astype(BF16)
            for b in range(blocks)
        ],
        axis=1,
    )
    packed = dot_nt(left_side, slot_hot[...])
    size = nvec * devices
    packed = packed[:size] + packed[size : 2 * size] + packed[2 * size :]
    for v in range(nvec):
        vsend[:, v, :] = packed[v * devices : (v + 1) * devices]
    exchange(vsend, rv, v_sem)
    sides_wait(kappa_sides, k_send, k_recv)
    strip = 4 * CY

    def laid(ref, get, every):
        for n, (dr, dc) in enumerate(every):
            value = get(dr, dc)
            for x in range(CX):
                at_row = ((dr + 1) * CX + x) * strip + (dc + 1) * CY
                ref[at_row : at_row + CY, :] = value[x * CY : (x + 1) * CY, :]

    every = SIDES + [(0, 0)]

    def valid(dr, dc):
        return (r + dr >= 0) & (r + dr < rows) & (c + dc >= 0) & (c + dc < cols)

    def stiffness(dr, dc):
        if (dr, dc) == (0, 0):
            return (6.0 + kappa_ref[...]) * 0.125
        return jnp.where(valid(dr, dc), (6.0 + kb[SIDES.index((dr, dc))]) * 0.125, 0.0)

    laid(coef, stiffness, every)
    laid(
        scale,
        lambda dr, dc: jnp.full((cells, LANES), jnp.where(valid(dr, dc), 0.125, 0.0), F32),
        every,
    )
    metas = settle(rm, devices - 1, m_sem)
    metas.wait_recv()
    for s in range(devices):
        lane_hot[:, s * LANES : (s + 1) * LANES] = (rm[s, 1:2, :] == lane_rows).astype(BF16)

    values = settle(rv, devices - 1, v_sem)
    values.wait_recv()

    cell_rows = iota((cells, LANES), 0).astype(F32)
    placed = []
    for s in range(devices):
        hit = rm[s, 0:1, :] == cell_rows
        bits = pieces(rv[s])
        placed.append(
            jnp.concatenate(
                [jnp.where(hit, bit[v : v + 1, :], 0.0) for bit in bits for v in range(nvec)],
                axis=0,
            ).astype(BF16)
        )
    field = dot_nt(jnp.concatenate(placed, axis=1), lane_hot[...])
    size = nvec * cells
    field = field[:size] + field[size : 2 * size] + field[2 * size :]
    for v in range(nvec):
        brick[v] = field[v * cells : (v + 1) * cells]
    corners = [n for n in range(len(SIDES)) if 0 not in SIDES[n]]
    for n in corners:
        held = corner_cells(*SIDES[n])
        for v in range(nvec):
            for i, (x, y) in enumerate(held):
                j, cell = v * len(held) + i, v * cells + x * CY + y
                corner[n, j // 4, j % 4 : j % 4 + 1, :] = field[cell : cell + 1]
    sides_start(field_sides, h_send, h_recv)
    gathered.wait_send()
    metas.wait_send()
    shares.wait_send()
    values.wait_send()
    sides_wait(field_sides, h_send, h_recv)

    def bricks(v, dr, dc):
        if (dr, dc) == (0, 0):
            return brick[v]
        return jnp.where(valid(dr, dc), hb[SIDES.index((dr, dc)), v], 0.0)

    for v in range(nvec):
        laid(
            ext.at[v],
            functools.partial(bricks, v),
            [near_side for near_side in every if 0 in near_side],
        )
        for n in corners:
            dr, dc = SIDES[n]
            held = corner_cells(-dr, -dc)
            for i, (x, y) in enumerate(held):
                j = v * len(held) + i
                at_row = ((dr + 1) * CX + x) * strip + (dc + 1) * CY + y
                ext[v, at_row : at_row + 1, :] = jnp.where(
                    valid(dr, dc), hc[n, j // 4, j % 4 : j % 4 + 1, :], 0.0
                )
        cur = ext[v]
        for step in range(4):
            mid = cur[strip:-strip]
            z = iota(mid.shape, 1)
            beside = cur[2 * strip :] + cur[: -2 * strip]
            beside += pltpu.roll(mid, 1, 0) + pltpu.roll(mid, mid.shape[0] - 1, 0)
            beside += jnp.where(z > 0, pltpu.roll(mid, 1, 1), 0.0)
            beside += jnp.where(z < LANES - 1, pltpu.roll(mid, LANES - 1, 1), 0.0)
            low = (step + 1) * strip
            span = slice(low, ext.shape[1] - low)
            cur = coef[span, :] * mid - scale[span, :] * beside
        out_ref[v] = cur.reshape(CX, strip, LANES)


def per_device(
    vectors, lr_left, lr_right, tile_rank, leaf_values, leaf_places, cluster_perm, kappa
):
    rows, cols = lax.axis_size("row"), lax.axis_size("col")
    devices = rows * cols
    nvec, _, points = vectors.shape
    tiles, kmax, tile = lr_left.shape[2:]
    nleaf, leaf = leaf_values.shape[2:4]
    cells, lanes = CX * CY, kappa.shape[2]
    taps = tiles * kmax
    strip, deep = 4 * CY, 3 * CX * 4 * CY
    vmem = pl.BlockSpec(memory_space=pltpu.VMEM)
    hbm = pl.BlockSpec(memory_space=pl.ANY)
    dma = pltpu.SemaphoreType.DMA
    out = pl.pallas_call(
        functools.partial(kernel, rows, cols, kmax, leaf),
        out_shape=pltpu.VMEM((nvec, CX, strip, lanes), F32),
        in_specs=[hbm] * 8,
        out_specs=vmem,
        scratch_shapes=[
            pltpu.SMEM((tiles,), jnp.int32),
            pltpu.SMEM((2, nleaf), jnp.int32),
            pltpu.VMEM((nleaf * nvec, leaf), F32),
            pltpu.VMEM((len(SIDES), 3 * nvec // 2, 4, lanes), F32),
            pltpu.VMEM((len(SIDES), 3 * nvec // 2, 4, lanes), F32),
            pltpu.VMEM((points // LANES, LANES), jnp.int32),
            pltpu.VMEM((cells, lanes), F32),
            pltpu.VMEM((taps, tile), BF16),
            pltpu.VMEM((taps, tile), BF16),
            pltpu.VMEM((nleaf, leaf, leaf), BF16),
            pltpu.VMEM((rows, nvec, points), BF16),
            pltpu.VMEM((TILE_COLS * nvec, tile), F32),
            pltpu.VMEM((cols, nvec, points), F32),
            pltpu.VMEM((cols - 1, nvec, points), F32),
            pltpu.VMEM((LANES, points), BF16),
            pltpu.VMEM((devices, 2, LANES), F32),
            pltpu.VMEM((devices, 2, LANES), F32),
            pltpu.VMEM((devices, nvec, LANES), F32),
            pltpu.VMEM((devices, nvec, LANES), F32),
            pltpu.VMEM((LANES, devices * LANES), BF16),
            pltpu.VMEM((nvec, cells, lanes), F32),
            pltpu.VMEM((len(SIDES), nvec, cells, lanes), F32),
            pltpu.VMEM((len(SIDES), cells, lanes), F32),
            pltpu.VMEM((nvec, deep, lanes), F32),
            pltpu.VMEM((deep, lanes), F32),
            pltpu.VMEM((deep, lanes), F32),
            dma((8,)), dma((2,)), dma((2,)), dma((2,)), dma((2,)),
            dma((len(SIDES),)), dma((len(SIDES),)), dma((len(SIDES),)), dma((len(SIDES),)),
        ],
        compiler_params=pltpu.CompilerParams(collective_id=0, has_side_effects=True),
    )(
        vectors.reshape(nvec, points),
        lr_right.reshape(taps, tile),
        lr_left.reshape(taps, tile),
        tile_rank.reshape(tiles),
        leaf_values.reshape(nleaf, leaf, leaf),
        leaf_places.reshape(nleaf, 2).T,
        cluster_perm.reshape(-1, LANES),
        kappa.reshape(cells, lanes),
    )
    return out[:, :, CY : 2 * CY, :]


def solution(mesh):
    in_specs = (
        P(None, "col", "row"),
        P("row", "col", None, None, None),
        P("row", "col", None, None, None),
        P("row", "col", None),
        P("row", "col", None, None, None),
        P("row", "col", None, None),
        P("row", None),
        P("row", "col", None),
    )
    out_specs = P(None, "row", "col", None)
    return jax.shard_map(
        per_device, mesh=mesh, in_specs=in_specs, out_specs=out_specs, check_vma=False
    )
```
